256 devices in a mesh: tm: 32 (over x_lo, z, core), tile: 8 (over x_hi, y).
Axes of the slice: x: 4 (x_hi: 2, x_lo: 2; x = x_hi * 2 + x_lo), y: 4, z: 8, core: 2. Of those that a mesh axis runs over, the one named last changes fastest.
Arguments:
- queries: bfloat16 [64, 16, 64, 2560], P('tm', 'tile'), may hold values from -40 to 40
- keys: bfloat16 [64, 16, 64, 2560], P('tm', 'tile'), may hold values from -6 to 6
- values: bfloat16 [64, 16, 64, 2560], P('tm', 'tile'), may hold values from -6 to 6
- neighbours: int32 [32, 8, 3], P('tm', 'tile'), may hold values from -1 to 30, as said below
- halo_rows: int32 [32, 8], P('tm', 'tile'), may hold values from 0 to 2, as said below
Outputs:
- attended: bfloat16 [64, 16, 64, 2560], P('tm', 'tile')
The draws below stay inside these ranges and needn't reach their ends.
Inputs may be any that keep to these rules, and one draw needn't show every extreme that they name: `neighbours`: for frame block b and tile t, the entries that are not -1 are distinct frame blocks from max(0, b - 5) to b - 1; lists hold 0 to 3 entries, and some list is full. `halo_rows`: some frame block and tile reads 2 rows.
All inputs are finite; a program needn't handle non-finite values.
Results may differ from the reference program's by a relative error of at most 0.0046.
Values may be sent and summed in bfloat16 or wider, within the bound.
A program may use at most 128 MiB of HBM per device.

```python
import math
import jax
import jax.numpy as jnp
from jax import lax

HEADS = 20
HD = 128
GRID_W = 64
FR_DEV = 2
TROWS = 2
HMAX = 2
NB = 3
WIN = 5
CHANNELS = 2560
BLOCKS = 32
TILES = 8
FRAMES = 64
GRID_H = 16


def drawn_pair(key):
    base = jax.random.fold_in(key, 11)
    query_seed, keys_seed = jax.random.split(base, 2)
    shape = (FRAMES, GRID_H, GRID_W, HEADS, HD)
    query_base = jnp.clip(jax.random.normal(query_seed, shape, jnp.float32), -6.0, 6.0)
    key_base = jnp.clip(jax.random.normal(keys_seed, shape, jnp.float32), -6.0, 6.0)
    flat_shape = (FRAMES, GRID_H, GRID_W, HEADS * HD)
    return (query_base.reshape(flat_shape), key_base.reshape(flat_shape))


def draw_queries(key, part):
    return drawn_pair(key)[0].astype(jnp.bfloat16)


def draw_keys(key, part):
    return drawn_pair(key)[1].astype(jnp.bfloat16)


def draw_neighbours(key, part):
    base = jax.random.fold_in(key, 31)
    bits_seed, length_seed = jax.random.split(base)
    random_bits = jax.random.randint(bits_seed, (BLOCKS, TILES, WIN), 0, 1 << 20)
    offsets = jnp.arange(1, WIN + 1, dtype=jnp.int32)
    block_pos = jnp.arange(BLOCKS, dtype=jnp.int32)[:, None, None]
    usable = block_pos - offsets[None, None, :] >= 0
    ranked = jnp.where(usable, random_bits * WIN + offsets - 1 + WIN, offsets - 1 + jnp.zeros_like(random_bits))
    top_vals, top_idx = lax.top_k(ranked, NB)
    chosen = top_idx.astype(jnp.int32) + 1
    list_length = jax.random.randint(length_seed, (BLOCKS, TILES), 0, NB + 1)
    list_length = list_length.at[BLOCKS - 1, 0].set(NB)
    slot_index = jnp.arange(NB, dtype=jnp.int32)[None, None, :]
    block_ids = block_pos - chosen
    kept_mask = (slot_index < list_length[:, :, None]) & (block_ids >= 0)
    return jnp.where(kept_mask, block_ids, -1).astype(jnp.int32)


def draw_halo_rows(key, part):
    widths = jax.random.randint(jax.random.fold_in(key, 23), (BLOCKS, TILES), 0, HMAX + 1)
    return widths.at[BLOCKS - 1, 0].set(HMAX).astype(jnp.int32)


def levels(key, shape, pieces, low, high):
    level, own = 1.0, jax.random.fold_in(key, 6)
    for axis_at, shards_of in pieces:
        draws = jnp.exp(jax.random.uniform(jax.random.fold_in(own, axis_at), (shards_of,), jnp.float32, low / len(pieces), high / len(pieces)))
        level = level * jnp.repeat(draws, shape[axis_at] // shards_of).reshape([-1 if axis == axis_at else 1 for axis in range(len(shape))])
    return level


def normal_values(key, shape, spread, bound, cuts=(), kind=jnp.bfloat16):
    factor_of = levels(key, shape, cuts, -0.22, 0.18) if cuts else 1.0
    array = jax.random.normal(key, shape, jnp.float32) * spread * factor_of
    return jnp.minimum(jnp.maximum(array, -bound), bound).astype(kind)


def setup_inputs(seed: int = 0) -> dict:
    key_list = jax.random.split(jax.random.key(seed), 6)
    return {
        "queries": draw_queries(jax.random.fold_in(key_list[5], 71), 0),
        "keys": draw_keys(jax.random.fold_in(key_list[5], 71), 0),
        "values": normal_values(key_list[2], (FRAMES, GRID_H, GRID_W, CHANNELS), 1.0, 6.0, ((0, 32), (1, 8))),
        "neighbours": draw_neighbours(jax.random.fold_in(key_list[5], 71), 0),
        "halo_rows": draw_halo_rows(jax.random.fold_in(key_list[5], 71), 0),
    }


def attend(query_rows, key_rows, value_rows, allowed):
    tokens, channels = query_rows.shape
    head_count = channels // HD
    key_count = key_rows.shape[0]
    query_heads = query_rows.astype(jnp.float32).reshape(tokens, head_count, HD)
    key_heads = key_rows.astype(jnp.float32).reshape(key_count, head_count, HD)
    value_heads = value_rows.astype(jnp.float32).reshape(key_count, head_count, HD)
    scores = jnp.einsum('qhd,khd->hqk', query_heads, key_heads) / math.sqrt(HD)
    scores = jnp.where(allowed[None], scores, -jnp.inf)
    maximum = lax.optimization_barrier(jnp.max(scores, axis=2, keepdims=True))
    weights = jnp.where(allowed[None], jnp.exp(scores - maximum), 0.0)
    totals = lax.optimization_barrier(jnp.sum(weights, axis=2))
    rounded = lax.optimization_barrier(weights.astype(jnp.bfloat16)).astype(jnp.float32)
    numerator = jnp.einsum('hqk,khd->qhd', rounded, value_heads)
    return (numerator / totals.T[:, :, None]).reshape(tokens, channels).astype(jnp.bfloat16)

def reference(queries, keys, values, neighbours, halo_rows):
    channels = queries.shape[3]
    tokens = FR_DEV * TROWS * GRID_W
    span_rows = TROWS + 2 * HMAX
    pad_keys = jnp.pad(keys, ((0, 0), (HMAX, HMAX), (0, 0), (0, 0)))
    pad_values = jnp.pad(values, ((0, 0), (HMAX, HMAX), (0, 0), (0, 0)))
    anchor = jnp.zeros((), jnp.int32)
    query_frame = lax.broadcasted_iota(jnp.int32, (FR_DEV, TROWS, GRID_W), 0).reshape(-1)
    key_frame = lax.broadcasted_iota(jnp.int32, (FR_DEV, span_rows, GRID_W), 0).reshape(-1)
    key_row = lax.broadcasted_iota(jnp.int32, (FR_DEV, span_rows, GRID_W), 1).reshape(-1)

    def one_device(device):
        block_index = (device // TILES).astype(jnp.int32)
        tile_index = (device % TILES).astype(jnp.int32)
        frame_start = (block_index * FR_DEV).astype(jnp.int32)
        row_start = (tile_index * TROWS).astype(jnp.int32)
        query_rows = lax.dynamic_slice(queries, (frame_start, row_start, anchor, anchor), (FR_DEV, TROWS, GRID_W, channels)).reshape(tokens, channels)
        own_keys = lax.dynamic_slice(pad_keys, (frame_start, row_start, anchor, anchor), (FR_DEV, span_rows, GRID_W, channels)).reshape(-1, channels)
        own_values = lax.dynamic_slice(pad_values, (frame_start, row_start, anchor, anchor), (FR_DEV, span_rows, GRID_W, channels)).reshape(-1, channels)
        listed = neighbours[block_index, tile_index]
        halo_reach = halo_rows[block_index, tile_index]

        def fetch_rows(block_id):
            start_frame = (jnp.maximum(block_id, 0) * FR_DEV).astype(jnp.int32)
            far_keys = lax.dynamic_slice(keys, (start_frame, row_start, anchor, anchor), (FR_DEV, TROWS, GRID_W, channels))
            far_values = lax.dynamic_slice(values, (start_frame, row_start, anchor, anchor), (FR_DEV, TROWS, GRID_W, channels))
            return (far_keys, far_values)
        far_keys, far_values = jax.vmap(fetch_rows)(listed)
        global_row = row_start - HMAX + key_row
        row_ok = (global_row >= 0) & (global_row < GRID_H) & (key_row >= HMAX - halo_reach) & (key_row < HMAX + TROWS + halo_reach)
        own_mask = (key_frame[None, :] <= query_frame[:, None]) & row_ok[None, :]
        slot_mask = jnp.repeat(listed >= 0, tokens)
        allowed = jnp.concatenate((own_mask, jnp.broadcast_to(slot_mask[None, :], (tokens, slot_mask.shape[0]))), axis=1)
        key_rows = jnp.concatenate((own_keys, far_keys.reshape(-1, channels)), axis=0)
        value_rows = jnp.concatenate((own_values, far_values.reshape(-1, channels)), axis=0)
        return attend(query_rows, key_rows, value_rows, allowed)
    results = lax.map(one_device, jnp.arange(BLOCKS * TILES, dtype=jnp.int32))
    results = results.reshape(BLOCKS, TILES, FR_DEV, TROWS, GRID_W, channels)
    return results.transpose(0, 2, 1, 3, 4, 5).reshape(FRAMES, GRID_H, GRID_W, channels)
```

```python
import functools
import math

import jax
import jax.numpy as jnp
from jax import lax
from jax.experimental import pallas as pl
from jax.experimental.pallas import tpu as pltpu
from jax.sharding import PartitionSpec as P

HD = 128
WIN = 5
BIG = 1e30
SCALE = math.log2(math.e) / math.sqrt(HD)
LAGS = (1, 2, 3, 4, 5, 6)
MESH = pl.DeviceIdType.MESH


def attend(parts):
    top = None
    for scores, _, groups in parts:
        for start, size, seen in groups:
            peak = jnp.max(scores[start : start + size], axis=0, keepdims=True)
            peak = jnp.where(seen, peak, -BIG)
            top = peak if top is None else jnp.maximum(top, peak)
    total, out = None, None
    for scores, value_t, groups in parts:
        pieces = []
        for start, size, seen in groups:
            shift = jnp.where(seen, top, BIG)
            weights = jnp.exp2((scores[start : start + size] - shift) * SCALE)
            added = jnp.sum(weights, axis=0, keepdims=True)
            total = added if total is None else total + added
            pieces.append(weights.astype(jnp.bfloat16))
        weights = pieces[0] if len(pieces) == 1 else jnp.concatenate(pieces, axis=0)
        product = jnp.dot(value_t, weights, preferred_element_type=jnp.float32)
        out = product if out is None else out + product
    return out, total, top


def scores_of(keys, queries):
    return lax.dot_general(
        keys, queries, (((1,), (1,)), ((), ())), preferred_element_type=jnp.float32
    )


def settle(total, top):
    empty = total == 0.0
    lse = jnp.where(empty, -BIG, top * SCALE + jnp.log2(jnp.where(empty, 1.0, total)))
    return lse, 1.0 / jnp.where(empty, 1.0, total)


def merge(lse_a, lse_b):
    top = jnp.maximum(lse_a, lse_b)
    wa, wb = jnp.exp2(lse_a - top), jnp.exp2(lse_b - top)
    both = wa + wb
    return wa / both, wb / both, top + jnp.log2(both)


def kernel(
    blocks,
    tiles,
    heads,
    q_ref,
    k_ref,
    v_ref,
    meta_ref,
    out_ref,
    qo,
    kvo,
    kvh,
    vt,
    vth,
    rq,
    ro,
    rl,
    so,
    sl,
    outs,
    om,
    rm,
    q_local,
    q_remote,
    kv_sem,
    meta_sem,
    halo_sem,
    m_sem,
    n_sem,
    l_sem,
    m_sent,
    n_sent,
    l_sent,
    x_sent,
    halo_sent,
    out_sem,
):
    chunks = 2 * heads
    me = lax.axis_index("tm")
    tile = lax.axis_index("tile")
    core = lax.rem(me, 2)
    other = 1 - core
    partner = {"tm": me + 1 - 2 * core}
    back = {"tm": lax.rem(me + blocks - 2, blocks)}
    ahead = {"tm": lax.rem(me + 2, blocks)}
    up = {"tile": lax.max(tile - 1, 0)}
    down = {"tile": lax.min(tile + 1, tiles - 1)}
    has_up = tile > 0
    has_down = tile < tiles - 1

    def remote(src, dst, sent, received, device):
        return pltpu.make_async_remote_copy(
            src_ref=src,
            dst_ref=dst,
            send_sem=sent,
            recv_sem=received,
            device_id=device,
            device_id_type=MESH,
        )

    def arrived(ref, sem):
        pltpu.make_async_copy(ref, ref, sem).wait()

    def column(half, h):
        return pl.ds(pl.multiple_of((half * heads + h) * HD, HD), HD)

    barrier = pltpu.get_barrier_semaphore()
    rings = ({"tile": lax.rem(tile + 1, tiles)}, {"tile": lax.rem(tile + tiles - 1, tiles)})
    for device in (partner, back, ahead) + rings:
        pl.semaphore_signal(barrier, inc=1, device_id=device, device_id_type=MESH)

    pltpu.make_async_copy(meta_ref, om.at[core], meta_sem.at[0]).start()

    def fetch_q(h, _):
        pltpu.make_async_copy(
            q_ref.at[:, :, column(core, h)], qo.at[h, :, core], q_local.at[h]
        ).start()
        return 0

    def fetch_kv(h, _):
        for i, ref in enumerate((k_ref, v_ref)):
            pltpu.make_async_copy(
                ref.at[:, column(core, h)], kvo.at[h, i, core], kv_sem.at[0]
            ).start()
        return 0

    lax.fori_loop(0, heads, fetch_q, 0)
    lax.fori_loop(0, heads, fetch_kv, 0)

    pl.semaphore_wait(barrier, 5)

    remote(meta_ref, om.at[core], x_sent.at[0], meta_sem.at[1], partner).start()

    def give_q(h, _):
        remote(
            q_ref.at[:, :, column(other, h)], qo.at[h, :, core], x_sent.at[1], q_remote.at[h], partner
        ).start()
        return 0

    def give_kv(h, _):
        for i, ref in enumerate((k_ref, v_ref)):
            remote(
                ref.at[:, column(other, h)], kvo.at[h, i, core], x_sent.at[2], kv_sem.at[1], partner
            ).start()
        return 0

    lax.fori_loop(0, heads, give_q, 0)
    lax.fori_loop(0, heads, give_kv, 0)

    @pl.when(jnp.logical_not(has_up))
    def _():
        def clear(h, _):
            kvh[0, h] = jnp.zeros(kvh.shape[2:], kvh.dtype)
            return 0

        lax.fori_loop(0, heads, clear, 0)

    @pl.when(jnp.logical_not(has_down))
    def _():
        def clear(h, _):
            kvh[1, h] = jnp.zeros(kvh.shape[2:], kvh.dtype)
            return 0

        lax.fori_loop(0, heads, clear, 0)

    def own_send(i):
        return remote(qo.at[i // 2, i % 2], rq.at[i, 0:2], m_sent.at[0], m_sem.at[0, i], back)

    def relay_one(i):
        return remote(rq.at[i, 0:2], rq.at[i, 2:4], m_sent.at[1], m_sem.at[1, i], back)

    def relay_two(i):
        return remote(rq.at[i, 2], rq.at[i, 4], m_sent.at[2], m_sem.at[2, i], back)

    def halo_to(direction, h, device):
        return remote(
            kvo.at[h], kvh.at[direction, h], halo_sent.at[direction], halo_sem.at[direction, h], device
        )

    slots = ((3, 5), (1, 3), (0, 1))

    def out_send(which, i):
        lo, hi = slots[which]
        return (
            remote(so.at[i, lo:hi], ro.at[i, lo:hi], n_sent.at[which], n_sem.at[which, i], ahead),
            remote(sl.at[i, lo:hi], rl.at[i, lo:hi], l_sent.at[which], l_sem.at[which, i], ahead),
        )

    def far(i, which, joined):
        lo, hi = slots[which]
        h = i // 2
        width = (hi - lo) * HD
        queries = rq[i, lo:hi].reshape(width, HD)
        seen = []
        for side in (2, 1):
            flags = [rm[j, j + side : j + side + 1, :] > 0.5 for j in range(lo, hi)]
            seen.append(jnp.concatenate([jnp.where(f, 1.0, 0.0) for f in flags], axis=1) > 0.5)
        parts = []
        for x in range(2):
            scores = scores_of(kvo[h, 0, x], queries)
            parts.append((scores, vt[h, x], [(0, scores.shape[0], seen[x])]))
        out, total, top = attend(parts)
        lse, scale = settle(total, top)
        if joined is not None:
            joined()
        for n, j in enumerate(range(lo, hi)):
            lanes = slice(n * HD, (n + 1) * HD)
            part, own_lse, own_scale = out[:, lanes], lse[:, lanes], scale[:, lanes]
            if joined is not None:
                wa, wb, new_lse = merge(own_lse, rl[i, j + 2])
                part = part * (own_scale * wa) + ro[i, j + 2].astype(jnp.float32) * wb
                own_lse = new_lse
            else:
                part = part * own_scale
            so[i, j] = part.astype(jnp.bfloat16)
            sl[i, j] = own_lse
        for copy in out_send(which, i):
            copy.start()

    def own(i):
        h, f = i // 2, i % 2
        second = jnp.full((1, HD), f, jnp.int32) > 0
        first = jnp.full((1, HD), f, jnp.int32) >= 0
        for x in range(2):
            queries = qo[h, f, x]
            reach_up, reach_down = om[x, 0:1, :], om[x, 7:8, :]
            parts = [
                (scores_of(kvo[h, 0, x], queries), vt[h, x], [(0, 128, first), (128, 128, second)])
            ]
            for direction, reach in ((0, reach_up), (1, reach_down)):
                groups = []
                for frame in range(2):
                    for row in range(2):
                        need = 2 - row if direction == 0 else 1 + row
                        seen = reach > need - 0.5
                        if frame:
                            seen = seen & second
                        groups.append((frame * 128 + row * 64, 64, seen))
                parts.append(
                    (scores_of(kvh[direction, h, 0, x], queries), vth[direction, x], groups)
                )
            if x == 1:
                parts.append(
                    (scores_of(kvo[h, 0, 0], queries), vt[h, 0], [(0, 256, om[1, 1:2, :] > 0.5)])
                )
            out, total, top = attend(parts)
            lse, scale = settle(total, top)
            wa, wb, _ = merge(lse, rl[i, x])
            whole = out * (scale * wa) + ro[i, x].astype(jnp.float32) * wb
            outs[h, f, x] = whole.T.astype(jnp.bfloat16)
        pltpu.make_async_copy(
            outs.at[h, f, core], out_ref.at[f, :, column(core, h)], out_sem.at[0]
        ).start()
        remote(
            outs.at[h, f, other],
            out_ref.at[f, :, column(core, h)],
            out_sem.at[1],
            out_sem.at[2],
            partner,
        ).start()

    def during(t, lag):
        i = t - lag
        return i, (i >= 0) & (i < chunks)

    def step(t, _):
        i2, live2 = during(t, LAGS[1])

        @pl.when(live2)
        def _():
            relay_one(i2).wait_recv()

            @pl.when(i2 == 0)
            def _():
                remote(rm.at[0:2], rm.at[2:4], x_sent.at[4], meta_sem.at[3], back).wait_recv()
                remote(rm.at[2], rm.at[4], x_sent.at[5], meta_sem.at[4], back).start()

            relay_two(i2).start()

        i1, live1 = during(t, LAGS[0])

        @pl.when(live1)
        def _():
            own_send(i1).wait_recv()

            @pl.when(i1 == 0)
            def _():
                remote(om, rm.at[0:2], x_sent.at[3], meta_sem.at[2], back).wait_recv()
                remote(rm.at[0:2], rm.at[2:4], x_sent.at[4], meta_sem.at[3], back).start()

            relay_one(i1).start()

        @pl.when(t < chunks)
        def _():
            h = t // 2

            @pl.when(t % 2 == 0)
            def _():
                arrived(qo.at[h, :, core], q_local.at[h])
                arrived(qo.at[h, :, other], q_remote.at[h])

            @pl.when(t == 0)
            def _():
                arrived(om.at[core], meta_sem.at[0])
                arrived(om.at[other], meta_sem.at[1])
                remote(om, rm.at[0:2], x_sent.at[3], meta_sem.at[2], back).start()

            own_send(t).start()

            @pl.when(t == 0)
            def _():
                arrived(kvo.at[:, :, core], kv_sem.at[0])
                arrived(kvo.at[:, :, other], kv_sem.at[1])

            @pl.when(t % 2 == 0)
            def _():
                @pl.when(has_down)
                def _():
                    halo_to(0, h, down).start()

                @pl.when(has_up)
                def _():
                    halo_to(1, h, up).start()

        i3, live3 = during(t, LAGS[2])

        @pl.when(live3)
        def _():
            @pl.when(i3 % 2 == 0)
            def _():
                for x in range(2):
                    vt[i3 // 2, x] = kvo[i3 // 2, 1, x].T

            relay_two(i3).wait_recv()

            @pl.when(i3 == 0)
            def _():
                remote(rm.at[2], rm.at[4], x_sent.at[5], meta_sem.at[4], back).wait_recv()

            far(i3, 0, None)

        for which in (1, 2):
            i, live = during(t, LAGS[2 + which])

            @pl.when(live)
            def _():
                def joined():
                    for copy in out_send(which - 1, i):
                        copy.wait_recv()

                far(i, which, joined)

        i6, live6 = during(t, LAGS[5])

        @pl.when(live6)
        def _():
            h = i6 // 2

            @pl.when(i6 % 2 == 0)
            def _():
                @pl.when(has_up)
                def _():
                    halo_to(0, h, down).wait_recv()

                @pl.when(has_down)
                def _():
                    halo_to(1, h, up).wait_recv()

                for direction in range(2):
                    for x in range(2):
                        vth[direction, x] = kvh[direction, h, 1, x].T

            for copy in out_send(2, i6):
                copy.wait_recv()
            own(i6)

        return 0

    lax.fori_loop(0, chunks + LAGS[5], step, 0)

    arrived(meta_ref, x_sent.at[0])
    arrived(qo.at[:, :, core], x_sent.at[1])
    arrived(kvo.at[:, :, core], x_sent.at[2])
    arrived(om, x_sent.at[3])
    arrived(rm.at[0:2], x_sent.at[4])
    arrived(rm.at[2], x_sent.at[5])
    arrived(qo, m_sent.at[0])
    arrived(rq.at[:, 0:2], m_sent.at[1])
    arrived(rq.at[:, 2], m_sent.at[2])
    for which, (lo, hi) in enumerate(slots):
        arrived(so.at[:, lo:hi], n_sent.at[which])
        arrived(sl.at[:, lo:hi], l_sent.at[which])

    @pl.when(has_down)
    def _():
        arrived(kvo, halo_sent.at[0])

    @pl.when(has_up)
    def _():
        arrived(kvo, halo_sent.at[1])

    for i in range(3):
        arrived(outs.at[:, :, 0], out_sem.at[i])


def local(blocks, tiles, queries, keys, values, neighbours, halo_rows):
    frames, rows, width, channels = queries.shape
    tokens = frames * rows * width
    heads = channels // HD // 2
    chunks = 2 * heads
    block = lax.axis_index("tm")
    tile = lax.axis_index("tile")
    listed = neighbours[0, 0]
    distance = jnp.arange(8, dtype=jnp.int32)
    hit = (listed[None, :] >= 0) & (listed[None, :] == block - distance[:, None])
    hit = jnp.any(hit, axis=1) & (distance >= 1) & (distance <= WIN)
    reach = halo_rows[0, 0]
    meta = jnp.where(hit, 1, 0)
    meta = jnp.where(distance == 0, jnp.where(tile > 0, reach, 0), meta)
    meta = jnp.where(distance == 7, jnp.where(tile < tiles - 1, reach, 0), meta)
    meta = jnp.broadcast_to(meta.astype(jnp.float32)[:, None], (8, HD))
    half = tokens // 2
    bf16, f32 = jnp.bfloat16, jnp.float32
    dma = pltpu.SemaphoreType.DMA
    result = pl.pallas_call(
        functools.partial(kernel, blocks, tiles, heads),
        out_shape=jax.ShapeDtypeStruct((2, half, channels), bf16),
        in_specs=[pl.BlockSpec(memory_space=pl.ANY)] * 3 + [pl.BlockSpec(memory_space=pltpu.VMEM)],
        out_specs=pl.BlockSpec(memory_space=pl.ANY),
        scratch_shapes=[
            pltpu.VMEM((heads, 2, 2, half, HD), bf16),
            pltpu.VMEM((heads, 2, 2, tokens, HD), bf16),
            pltpu.VMEM((2, heads, 2, 2, tokens, HD), bf16),
            pltpu.VMEM((heads, 2, HD, tokens), bf16),
            pltpu.VMEM((2, 2, HD, tokens), bf16),
            pltpu.VMEM((chunks, 5, half, HD), bf16),
            pltpu.VMEM((chunks, 5, HD, half), bf16),
            pltpu.VMEM((chunks, 5, 1, half), f32),
            pltpu.VMEM((chunks, 5, HD, half), bf16),
            pltpu.VMEM((chunks, 5, 1, half), f32),
            pltpu.VMEM((heads, 2, 2, half, HD), bf16),
            pltpu.VMEM((2, 8, HD), f32),
            pltpu.VMEM((5, 8, HD), f32),
            dma((heads,)),
            dma((heads,)),
            dma((2,)),
            dma((5,)),
            dma((2, heads)),
            dma((3, chunks)),
            dma((3, chunks)),
            dma((3, chunks)),
            dma((3,)),
            dma((3,)),
            dma((3,)),
            dma((6,)),
            dma((2,)),
            dma((3,)),
        ],
        compiler_params=pltpu.CompilerParams(
            collective_id=0, has_side_effects=True, vmem_limit_bytes=48 * 1024 * 1024
        ),
    )(
        queries.reshape(2, half, channels),
        keys.reshape(tokens, channels),
        values.reshape(tokens, channels),
        meta,
    )
    return result.reshape(frames, rows, width, channels)


def solution(mesh):
    body = functools.partial(local, mesh.shape["tm"], mesh.shape["tile"])
    return jax.shard_map(
        body,
        mesh=mesh,
        in_specs=(
            P("tm", "tile", None, None),
            P("tm", "tile", None, None),
            P("tm", "tile", None, None),
            P("tm", "tile", None),
            P("tm", "tile"),
        ),
        out_specs=P("tm", "tile", None, None),
        check_vma=False,
    )
```

```python
import functools
import math

import jax
import jax.numpy as jnp
from jax import lax
from jax.experimental import pallas as pl
from jax.experimental.pallas import tpu as pltpu
from jax.sharding import PartitionSpec as P

HD = 128
BIG = 1e30
SCALE = math.log2(math.e) / math.sqrt(HD)
LAGS = (2, 4, 6, 8, 10, 12)
RELAY = 5
MESH = pl.DeviceIdType.MESH


def attend(parts):
    top = None
    for scores, _, groups in parts:
        for start, size, seen in groups:
            peak = jnp.max(scores[start : start + size], axis=0, keepdims=True)
            peak = jnp.where(seen, peak, -BIG)
            top = peak if top is None else jnp.maximum(top, peak)
    total, out = None, None
    for scores, value_t, groups in parts:
        pieces = []
        for start, size, seen in groups:
            shift = jnp.where(seen, top, BIG)
            weights = jnp.exp2((scores[start : start + size] - shift) * SCALE)
            added = jnp.sum(weights, axis=0, keepdims=True)
            total = added if total is None else total + added
            pieces.append(weights.astype(jnp.bfloat16))
        weights = pieces[0] if len(pieces) == 1 else jnp.concatenate(pieces, axis=0)
        product = jnp.dot(value_t, weights, preferred_element_type=jnp.float32)
        out = product if out is None else out + product
    return out, total, top


def scores_of(keys, queries):
    return lax.dot_general(
        keys, queries, (((1,), (1,)), ((), ())), preferred_element_type=jnp.float32
    )


def settle(total, top):
    empty = total == 0.0
    lse = jnp.where(empty, -BIG, top * SCALE + jnp.log2(jnp.where(empty, 1.0, total)))
    return lse, 1.0 / jnp.where(empty, 1.0, total)


def merge(lse_a, lse_b):
    top = jnp.maximum(lse_a, lse_b)
    wa, wb = jnp.exp2(lse_a - top), jnp.exp2(lse_b - top)
    both = wa + wb
    return wa / both, wb / both, top + jnp.log2(both)


def kernel(
    blocks,
    tiles,
    heads,
    q_ref,
    k_ref,
    v_ref,
    list_ref,
    reach_ref,
    out_ref,
    qo,
    kvo,
    kvh,
    vt,
    vth,
    rq,
    ro,
    rl,
    so,
    sl,
    outs,
    om,
    rm,
    q_local,
    q_remote,
    kv_sem,
    meta_sem,
    halo_sem,
    m_sem,
    n_sem,
    l_sem,
    m_sent,
    n_sent,
    l_sent,
    x_sent,
    halo_sent,
    out_sem,
):
    chunks = 2 * heads
    me = lax.axis_index("tm")
    tile = lax.axis_index("tile")
    core = lax.rem(me, 2)
    other = 1 - core
    partner = {"tm": me + 1 - 2 * core}
    back = {"tm": lax.rem(me + blocks - 2, blocks)}
    ahead = {"tm": lax.rem(me + 2, blocks)}
    across = lax.rem(me + blocks // 2, blocks)
    has_up = tile > 0
    has_down = tile < tiles - 1
    has_ahead = me < blocks - 2
    has_back = me >= 2
    upper, lower, last = tiles // 2 - 1, tiles // 2, tiles - 1
    chip = me // 2
    chips = blocks // 2
    at_end = (chip == 0) | (chip == chips - 1)
    at_edge = at_end | (chip == chips // 2 - 1) | (chip == chips // 2)
    detours = at_edge & ((tile == upper) | (tile == lower))
    relays = at_edge & ((tile == 0) | (tile == last))
    takes_up = has_up | (relays & (tile == 0))
    takes_down = has_down | (relays & (tile == last))

    def remote(src, dst, sent, received, device):
        return pltpu.make_async_remote_copy(
            src_ref=src,
            dst_ref=dst,
            send_sem=sent,
            recv_sem=received,
            device_id=device,
            device_id_type=MESH,
        )

    def arrived(ref, sem):
        pltpu.make_async_copy(ref, ref, sem).wait()

    def column(half, h):
        return pl.ds(pl.multiple_of((half * heads + h) * HD, HD), HD)

    barrier = pltpu.get_barrier_semaphore()
    rings = ({"tile": lax.rem(tile + 1, tiles)}, {"tile": lax.rem(tile + tiles - 1, tiles)})
    for device in (partner, back, ahead) + rings:
        pl.semaphore_signal(barrier, inc=1, device_id=device, device_id_type=MESH)

    @pl.when(detours)
    def _():
        for n in (0, tiles - 1):
            pl.semaphore_signal(
                barrier, inc=1, device_id={"tm": across, "tile": n}, device_id_type=MESH
            )

    @pl.when(relays)
    def _():
        for n in (upper, lower):
            pl.semaphore_signal(
                barrier, inc=1, device_id={"tm": across, "tile": n}, device_id_type=MESH
            )

    def fetch_q(h, _):
        pltpu.make_async_copy(
            q_ref.at[:, :, column(core, h)], qo.at[h, :, core], q_local.at[h]
        ).start()
        return 0

    def fetch_kv(h, _):
        for i, ref in enumerate((k_ref, v_ref)):
            pltpu.make_async_copy(
                ref.at[:, column(core, h)], kvo.at[h, i, core], kv_sem.at[0]
            ).start()
        return 0

    lax.fori_loop(0, heads, fetch_q, 0)
    lax.fori_loop(0, heads, fetch_kv, 0)

    distance = lax.broadcasted_iota(jnp.int32, (8, HD), 0)
    meta = jnp.zeros((8, HD), jnp.float32)
    for n in range(list_ref.shape[0]):
        block = list_ref[n]
        meta = jnp.where(distance == jnp.where(block >= 0, me - block, 0), 1.0, meta)
    reach = reach_ref[0].astype(jnp.float32)
    meta = jnp.where(distance == 0, jnp.where(has_up, reach, 0.0), meta)
    meta = jnp.where(distance == 7, jnp.where(has_down, reach, 0.0), meta)
    om[core] = meta

    @pl.when(jnp.logical_not(has_ahead))
    def _():
        rm[...] = jnp.zeros(rm.shape, rm.dtype)

        def clear(i, _):
            rq[i] = jnp.zeros(rq.shape[1:], rq.dtype)
            return 0

        lax.fori_loop(0, chunks, clear, 0)

    @pl.when(jnp.logical_not(has_back))
    def _():
        def clear(i, _):
            ro[i] = jnp.zeros(ro.shape[1:], ro.dtype)
            rl[i] = jnp.full(rl.shape[1:], -BIG, rl.dtype)
            return 0

        lax.fori_loop(0, chunks, clear, 0)

    @pl.when(detours | relays)
    def _():
        pl.semaphore_wait(barrier, 7)

    @pl.when(jnp.logical_not(detours | relays))
    def _():
        pl.semaphore_wait(barrier, 5)

    remote(om.at[core], om.at[core], x_sent.at[0], meta_sem.at[0], partner).start()

    def give_q(h, _):
        remote(
            q_ref.at[:, :, column(other, h)], qo.at[h, :, core], x_sent.at[1], q_remote.at[h], partner
        ).start()
        return 0

    def give_kv(h, _):
        for i, ref in enumerate((k_ref, v_ref)):
            remote(
                ref.at[:, column(other, h)], kvo.at[h, i, core], x_sent.at[2], kv_sem.at[1], partner
            ).start()
        return 0

    lax.fori_loop(0, heads, give_q, 0)
    lax.fori_loop(0, heads, give_kv, 0)

    @pl.when(jnp.logical_not(takes_up))
    def _():
        def clear(h, _):
            kvh[0, h] = jnp.zeros(kvh.shape[2:], kvh.dtype)
            return 0

        lax.fori_loop(0, heads, clear, 0)

    @pl.when(jnp.logical_not(takes_down))
    def _():
        def clear(h, _):
            kvh[1, h] = jnp.zeros(kvh.shape[2:], kvh.dtype)
            return 0

        lax.fori_loop(0, heads, clear, 0)

    def own_send(i):
        return remote(qo.at[i // 2, i % 2], rq.at[i, 0:2], m_sent.at[0], m_sem.at[0, i], back)

    def relay_one(i):
        return remote(rq.at[i, 0:2], rq.at[i, 2:4], m_sent.at[1], m_sem.at[1, i], back)

    def relay_two(i):
        return remote(rq.at[i, 2], rq.at[i, 4], m_sent.at[2], m_sem.at[2, i], back)

    def halo(direction, h, device, src=None):
        return remote(
            kvo.at[h] if src is None else src,
            kvh.at[direction, h],
            halo_sent.at[0 if src is None else 1],
            halo_sem.at[direction, h],
            device,
        )

    down = {"tm": me, "tile": tile + 1}
    up = {"tm": me, "tile": tile - 1}

    def opposite(n):
        return {"tm": across, "tile": n}

    def halo_out(h):
        @pl.when(has_down & jnp.logical_not(detours & (tile == upper)))
        def _():
            halo(0, h, down).start()

        @pl.when(has_up & jnp.logical_not(detours & (tile == lower)))
        def _():
            halo(1, h, up).start()

        by_last = (at_end & (tile == upper)) | (jnp.logical_not(at_end) & (tile == lower))

        @pl.when(detours & by_last)
        def _():
            halo(1, h, opposite(last)).start()

        @pl.when(detours & jnp.logical_not(by_last))
        def _():
            halo(0, h, opposite(0)).start()

    def halo_relay(h):
        for held, edge in ((0, 0), (1, last)):

            @pl.when(relays & (tile == edge))
            def _():
                halo(held, h, partner).wait_recv()

            for end in (True, False):
                onto = held if end else 1 - held

                @pl.when(relays & (tile == edge) & (at_end if end else jnp.logical_not(at_end)))
                def _():
                    halo(onto, h, opposite(upper if onto else lower), kvh.at[held, h]).start()

    def halo_in(h):
        @pl.when(has_up)
        def _():
            halo(0, h, partner).wait_recv()

        @pl.when(has_down)
        def _():
            halo(1, h, partner).wait_recv()

    slots = ((3, 5), (1, 3), (0, 1))

    def out_send(which, i):
        lo, hi = slots[which]
        return (
            remote(so.at[i, lo:hi], ro.at[i, lo:hi], n_sent.at[which], n_sem.at[which, i], ahead),
            remote(sl.at[i, lo:hi], rl.at[i, lo:hi], l_sent.at[which], l_sem.at[which, i], ahead),
        )

    def join(which, i):
        @pl.when(has_back)
        def _():
            for copy in out_send(which, i):
                copy.wait_recv()

    def far(i, which):
        lo, hi = slots[which]
        h = i // 2
        width = (hi - lo) * HD
        queries = rq[i, lo:hi].reshape(width, HD)
        seen = []
        for side in (2, 1):
            flags = [rm[j, j + side : j + side + 1, :] > 0.5 for j in range(lo, hi)]
            seen.append(jnp.concatenate([jnp.where(f, 1.0, 0.0) for f in flags], axis=1) > 0.5)
        parts = []
        for x in range(2):
            scores = scores_of(kvo[h, 0, x], queries)
            parts.append((scores, vt[h, x], [(0, scores.shape[0], seen[x])]))
        out, total, top = attend(parts)
        lse, scale = settle(total, top)
        if which:
            join(which - 1, i)
        for n, j in enumerate(range(lo, hi)):
            lanes = slice(n * HD, (n + 1) * HD)
            part, own_lse, own_scale = out[:, lanes], lse[:, lanes], scale[:, lanes]
            if which:
                wa, wb, new_lse = merge(own_lse, rl[i, j + 2])
                part = part * (own_scale * wa) + ro[i, j + 2].astype(jnp.float32) * wb
                own_lse = new_lse
            else:
                part = part * own_scale
            so[i, j] = part.astype(jnp.bfloat16)
            sl[i, j] = own_lse
        @pl.when(has_ahead)
        def _():
            for copy in out_send(which, i):
                copy.start()

    def own(i):
        h, f = i // 2, i % 2
        second = jnp.full((1, HD), f, jnp.int32) > 0
        first = jnp.full((1, HD), f, jnp.int32) >= 0
        for x in range(2):
            queries = qo[h, f, x]
            reach_up, reach_down = om[x, 0:1, :], om[x, 7:8, :]
            parts = [
                (scores_of(kvo[h, 0, x], queries), vt[h, x], [(0, 128, first), (128, 128, second)])
            ]
            for direction, reach in ((0, reach_up), (1, reach_down)):
                groups = []
                for frame in range(2):
                    for row in range(2):
                        need = 2 - row if direction == 0 else 1 + row
                        seen = reach > need - 0.5
                        if frame:
                            seen = seen & second
                        groups.append((frame * 128 + row * 64, 64, seen))
                parts.append(
                    (scores_of(kvh[direction, h, 0, x], queries), vth[direction, x], groups)
                )
            if x == 1:
                parts.append(
                    (scores_of(kvo[h, 0, 0], queries), vt[h, 0], [(0, 256, om[1, 1:2, :] > 0.5)])
                )
            out, total, top = attend(parts)
            lse, scale = settle(total, top)
            if x == 0:
                join(2, i)
            wa, wb, _ = merge(lse, rl[i, x])
            whole = out * (scale * wa) + ro[i, x].astype(jnp.float32) * wb
            outs[h, f, x] = whole.T.astype(jnp.bfloat16)
        pltpu.make_async_copy(
            outs.at[h, f, core], out_ref.at[f, :, column(core, h)], out_sem.at[0]
        ).start()
        remote(
            outs.at[h, f, other],
            out_ref.at[f, :, column(core, h)],
            out_sem.at[1],
            out_sem.at[2],
            partner,
        ).start()

    def during(t, lag):
        i = t - lag
        return i, (i >= 0) & (i < chunks)

    def meta_send(n):
        src, dst = ((om, rm.at[0:2]), (rm.at[0:2], rm.at[2:4]), (rm.at[2], rm.at[4]))[n]
        return remote(src, dst, x_sent.at[3 + n], meta_sem.at[1 + n], back)

    sends = (own_send, relay_one, relay_two)

    def pass_back(t, n):
        i, live = (t, t < chunks) if n == 0 else during(t, LAGS[n - 1])

        if n:

            @pl.when(live & has_ahead)
            def _():
                sends[n - 1](i).wait_recv()

                @pl.when(i == 0)
                def _():
                    meta_send(n - 1).wait_recv()

        @pl.when(live & has_back)
        def _():
            @pl.when(i == 0)
            def _():
                meta_send(n).start()

            sends[n](i).start()

    def step(t, _):
        @pl.when((t < chunks) & (t % 2 == 0))
        def _():
            arrived(qo.at[t // 2, :, core], q_local.at[t // 2])
            arrived(qo.at[t // 2, :, other], q_remote.at[t // 2])

        @pl.when(t == 0)
        def _():
            arrived(om.at[other], meta_sem.at[0])

        for n in (2, 1, 0):
            pass_back(t, n)

        @pl.when(t == 0)
        def _():
            arrived(kvo.at[:, :, core], kv_sem.at[0])
            arrived(kvo.at[:, :, other], kv_sem.at[1])

        @pl.when((t < chunks) & (t % 2 == 0))
        def _():
            halo_out(t // 2)

        ih, liveh = during(t, RELAY)

        @pl.when(liveh & (ih % 2 == 0))
        def _():
            halo_relay(ih // 2)

        i3, live3 = during(t, LAGS[2])

        @pl.when(live3)
        def _():
            @pl.when(i3 % 2 == 0)
            def _():
                for x in range(2):
                    vt[i3 // 2, x] = kvo[i3 // 2, 1, x].T

            @pl.when(has_ahead)
            def _():
                relay_two(i3).wait_recv()

                @pl.when(i3 == 0)
                def _():
                    meta_send(2).wait_recv()

            far(i3, 0)

        for which in (1, 2):
            i, live = during(t, LAGS[2 + which])

            @pl.when(live)
            def _():
                far(i, which)

        i6, live6 = during(t, LAGS[5])

        @pl.when(live6)
        def _():
            h = i6 // 2

            @pl.when(i6 % 2 == 0)
            def _():
                halo_in(h)
                for direction in range(2):
                    for x in range(2):
                        vth[direction, x] = kvh[direction, h, 1, x].T

            own(i6)

        return 0

    lax.fori_loop(0, chunks + LAGS[5], step, 0)

    arrived(om.at[core], x_sent.at[0])
    arrived(qo.at[:, :, core], x_sent.at[1])
    arrived(kvo.at[:, :, core], x_sent.at[2])

    @pl.when(has_back)
    def _():
        arrived(om, x_sent.at[3])
        arrived(rm.at[0:2], x_sent.at[4])
        arrived(rm.at[2], x_sent.at[5])
        arrived(qo, m_sent.at[0])
        arrived(rq.at[:, 0:2], m_sent.at[1])
        arrived(rq.at[:, 2], m_sent.at[2])

    @pl.when(has_ahead)
    def _():
        for which, (lo, hi) in enumerate(slots):
            arrived(so.at[:, lo:hi], n_sent.at[which])
            arrived(sl.at[:, lo:hi], l_sent.at[which])

    @pl.when(has_down & has_up)
    def _():
        arrived(kvh, halo_sent.at[0])

    @pl.when(jnp.logical_not(has_down & has_up))
    def _():
        arrived(kvo, halo_sent.at[0])

    @pl.when(relays)
    def _():
        arrived(kvo, halo_sent.at[1])

    for i in range(3):
        arrived(outs.at[:, :, 0], out_sem.at[i])


def local(blocks, tiles, queries, keys, values, neighbours, halo_rows):
    frames, rows, width, channels = queries.shape
    tokens = frames * rows * width
    heads = channels // HD // 2
    chunks = 2 * heads
    half = tokens // 2
    bf16, f32 = jnp.bfloat16, jnp.float32
    dma = pltpu.SemaphoreType.DMA
    result = pl.pallas_call(
        functools.partial(kernel, blocks, tiles, heads),
        out_shape=jax.ShapeDtypeStruct((2, half, channels), bf16),
        in_specs=[pl.BlockSpec(memory_space=pl.ANY)] * 3
        + [pl.BlockSpec(memory_space=pltpu.SMEM)] * 2,
        out_specs=pl.BlockSpec(memory_space=pl.ANY),
        scratch_shapes=[
            pltpu.VMEM((heads, 2, 2, half, HD), bf16),
            pltpu.VMEM((heads, 2, 2, tokens, HD), bf16),
            pltpu.VMEM((2, heads, 2, 2, tokens, HD), bf16),
            pltpu.VMEM((heads, 2, HD, tokens), bf16),
            pltpu.VMEM((2, 2, HD, tokens), bf16),
            pltpu.VMEM((chunks, 5, half, HD), bf16),
            pltpu.VMEM((chunks, 5, HD, half), bf16),
            pltpu.VMEM((chunks, 5, 1, half), f32),
            pltpu.VMEM((chunks, 5, HD, half), bf16),
            pltpu.VMEM((chunks, 5, 1, half), f32),
            pltpu.VMEM((heads, 2, 2, half, HD), bf16),
            pltpu.VMEM((2, 8, HD), f32),
            pltpu.VMEM((5, 8, HD), f32),
            dma((heads,)),
            dma((heads,)),
            dma((2,)),
            dma((4,)),
            dma((2, heads)),
            dma((3, chunks)),
            dma((3, chunks)),
            dma((3, chunks)),
            dma((3,)),
            dma((3,)),
            dma((3,)),
            dma((6,)),
            dma((2,)),
            dma((3,)),
        ],
        compiler_params=pltpu.CompilerParams(
            collective_id=0, has_side_effects=True, vmem_limit_bytes=62 * 1024 * 1024
        ),
    )(
        queries.reshape(2, half, channels),
        keys.reshape(tokens, channels),
        values.reshape(tokens, channels),
        neighbours.reshape(-1),
        halo_rows.reshape(-1),
    )
    return result.reshape(frames, rows, width, channels)


def solution(mesh):
    body = functools.partial(local, mesh.shape["tm"], mesh.shape["tile"])
    return jax.shard_map(
        body,
        mesh=mesh,
        in_specs=(
            P("tm", "tile", None, None),
            P("tm", "tile", None, None),
            P("tm", "tile", None, None),
            P("tm", "tile", None),
            P("tm", "tile"),
        ),
        out_specs=P("tm", "tile", None, None),
        check_vma=False,
    )
```

```python
import functools
import math

import jax
import jax.numpy as jnp
from jax import lax
from jax.experimental import pallas as pl
from jax.experimental.pallas import tpu as pltpu
from jax.sharding import PartitionSpec as P

HD = 128
BIG = 1e30
SCALE = math.log2(math.e) / math.sqrt(HD)
AHEAD = 2
KV_STEP = 7
LAGS = (0, 2, 3, 5, 7, 9)
RELAY = 4
MESH = pl.DeviceIdType.MESH


def attend(parts):
    top = None
    for scores, _, groups in parts:
        for start, size, seen in groups:
            peak = jnp.max(scores[start : start + size], axis=0, keepdims=True)
            peak = jnp.where(seen, peak, -BIG)
            top = peak if top is None else jnp.maximum(top, peak)
    total, out = None, None
    for scores, value_t, groups in parts:
        pieces = []
        for start, size, seen in groups:
            shift = jnp.where(seen, top, BIG)
            weights = jnp.exp2((scores[start : start + size] - shift) * SCALE)
            added = jnp.sum(weights, axis=0, keepdims=True)
            total = added if total is None else total + added
            pieces.append(weights.astype(jnp.bfloat16))
        weights = pieces[0] if len(pieces) == 1 else jnp.concatenate(pieces, axis=0)
        product = jnp.dot(value_t, weights, preferred_element_type=jnp.float32)
        out = product if out is None else out + product
    return out, total, top


def scores_of(keys, queries):
    return lax.dot_general(
        keys, queries, (((1,), (1,)), ((), ())), preferred_element_type=jnp.float32
    )


def settle(total, top):
    empty = total == 0.0
    lse = jnp.where(empty, -BIG, top * SCALE + jnp.log2(jnp.where(empty, 1.0, total)))
    return lse, 1.0 / jnp.where(empty, 1.0, total)


def merge(lse_a, lse_b):
    top = jnp.maximum(lse_a, lse_b)
    wa, wb = jnp.exp2(lse_a - top), jnp.exp2(lse_b - top)
    both = wa + wb
    return wa / both, wb / both, top + jnp.log2(both)


def kernel(
    blocks,
    tiles,
    heads,
    q_ref,
    k_ref,
    v_ref,
    list_ref,
    reach_ref,
    out_ref,
    qo,
    kvo,
    kvh,
    vt,
    vth,
    rq,
    ro,
    rl,
    so,
    sl,
    outs,
    om,
    rm,
    rk,
    q_local,
    q_remote,
    kv_sem,
    meta_sem,
    halo_sem,
    m_sem,
    n_sem,
    l_sem,
    m_sent,
    n_sent,
    l_sent,
    x_sent,
    halo_sent,
    k_sem,
    k_sent,
    out_sem,
):
    kv_head = heads - 1
    chunks = 2 * kv_head
    me = lax.axis_index("tm")
    tile = lax.axis_index("tile")
    core = lax.rem(me, 2)
    other = 1 - core
    partner = {"tm": me + 1 - 2 * core}
    back = {"tm": lax.rem(me + blocks - 2, blocks)}
    ahead = {"tm": lax.rem(me + 2, blocks)}
    across = lax.rem(me + blocks // 2, blocks)
    has_up = tile > 0
    has_down = tile < tiles - 1
    has_ahead = me < blocks - 2
    has_back = me >= 2
    upper, lower, last = tiles // 2 - 1, tiles // 2, tiles - 1
    chip = me // 2
    chips = blocks // 2
    at_end = (chip == 0) | (chip == chips - 1)
    at_edge = at_end | (chip == chips // 2 - 1) | (chip == chips // 2)
    detours = at_edge & ((tile == upper) | (tile == lower))
    relays = at_edge & ((tile == 0) | (tile == last))
    takes_up = has_up | (relays & (tile == 0))
    takes_down = has_down | (relays & (tile == last))

    def remote(src, dst, sent, received, device):
        return pltpu.make_async_remote_copy(
            src_ref=src,
            dst_ref=dst,
            send_sem=sent,
            recv_sem=received,
            device_id=device,
            device_id_type=MESH,
        )

    def arrived(ref, sem):
        pltpu.make_async_copy(ref, ref, sem).wait()

    def column(half, h):
        return pl.ds(pl.multiple_of((half * heads + h) * HD, HD), HD)

    barrier = pltpu.get_barrier_semaphore()
    rings = ({"tile": lax.rem(tile + 1, tiles)}, {"tile": lax.rem(tile + tiles - 1, tiles)})
    for device in (partner, back, ahead) + rings:
        pl.semaphore_signal(barrier, inc=1, device_id=device, device_id_type=MESH)

    @pl.when(detours)
    def _():
        for n in (0, tiles - 1):
            pl.semaphore_signal(
                barrier, inc=1, device_id={"tm": across, "tile": n}, device_id_type=MESH
            )

    @pl.when(relays)
    def _():
        for n in (upper, lower):
            pl.semaphore_signal(
                barrier, inc=1, device_id={"tm": across, "tile": n}, device_id_type=MESH
            )

    def fetch_q(h, _):
        pltpu.make_async_copy(
            q_ref.at[:, :, column(core, h)], qo.at[h, :, core], q_local.at[h]
        ).start()
        return 0

    def fetch_kv(h, _):
        for i, ref in enumerate((k_ref, v_ref)):
            pltpu.make_async_copy(
                ref.at[:, column(core, h)], kvo.at[h, i, core], kv_sem.at[0]
            ).start()
        return 0

    lax.fori_loop(0, heads, fetch_q, 0)
    lax.fori_loop(0, heads, fetch_kv, 0)

    distance = lax.broadcasted_iota(jnp.int32, (8, HD), 0)
    meta = jnp.zeros((8, HD), jnp.float32)
    for n in range(list_ref.shape[0]):
        block = list_ref[n]
        meta = jnp.where(distance == jnp.where(block >= 0, me - block, 0), 1.0, meta)
    reach = reach_ref[0].astype(jnp.float32)
    meta = jnp.where(distance == 0, jnp.where(has_up, reach, 0.0), meta)
    meta = jnp.where(distance == 7, jnp.where(has_down, reach, 0.0), meta)
    om[core] = meta

    @pl.when(jnp.logical_not(has_ahead))
    def _():
        rm[...] = jnp.zeros(rm.shape, rm.dtype)

        def clear(i, _):
            rq[i] = jnp.zeros(rq.shape[1:], rq.dtype)
            return 0

        lax.fori_loop(0, chunks, clear, 0)

    @pl.when(jnp.logical_not(has_back))
    def _():
        def clear(i, _):
            ro[i] = jnp.zeros(ro.shape[1:], ro.dtype)
            rl[i] = jnp.full(rl.shape[1:], -BIG, rl.dtype)
            return 0

        lax.fori_loop(0, chunks, clear, 0)
        for n in range(rk.shape[0]):
            for i in range(2):
                rk[n, i] = jnp.zeros(rk.shape[2:], rk.dtype)

    @pl.when(detours | relays)
    def _():
        pl.semaphore_wait(barrier, 7)

    @pl.when(jnp.logical_not(detours | relays))
    def _():
        pl.semaphore_wait(barrier, 5)

    remote(om.at[core], om.at[core], x_sent.at[0], meta_sem.at[0], partner).start()

    def give_q(h, _):
        remote(
            q_ref.at[:, :, column(other, h)], qo.at[h, :, core], x_sent.at[1], q_remote.at[h], partner
        ).start()
        return 0

    def give_kv(h, _):
        for i, ref in enumerate((k_ref, v_ref)):
            remote(
                ref.at[:, column(other, h)], kvo.at[h, i, core], x_sent.at[2], kv_sem.at[1], partner
            ).start()
        return 0

    lax.fori_loop(0, heads, give_q, 0)

    def own_send(i):
        return remote(qo.at[i // 2, i % 2], rq.at[i, 0:2], m_sent.at[0], m_sem.at[0, i], back)

    def meta_send(n):
        src, dst = ((om, rm.at[0:2]), (rm.at[0:2], rm.at[2:4]), (rm.at[2], rm.at[4]))[n]
        return remote(src, dst, x_sent.at[3 + n], meta_sem.at[1 + n], back)

    def await_queries(h):
        arrived(qo.at[h, :, core], q_local.at[h])
        arrived(qo.at[h, :, other], q_remote.at[h])

    for i in range(AHEAD):
        if i % 2 == 0:
            await_queries(i // 2)

        @pl.when(has_back)
        def _():
            own_send(i).start()

    lax.fori_loop(0, heads, give_kv, 0)
    arrived(om.at[other], meta_sem.at[0])

    @pl.when(has_back)
    def _():
        meta_send(0).start()

    @pl.when(jnp.logical_not(takes_up))
    def _():
        def clear(h, _):
            kvh[0, h] = jnp.zeros(kvh.shape[2:], kvh.dtype)
            return 0

        lax.fori_loop(0, heads, clear, 0)

    @pl.when(jnp.logical_not(takes_down))
    def _():
        def clear(h, _):
            kvh[1, h] = jnp.zeros(kvh.shape[2:], kvh.dtype)
            return 0

        lax.fori_loop(0, heads, clear, 0)

    def relay_one(i):
        return remote(rq.at[i, 0:2], rq.at[i, 2:4], m_sent.at[1], m_sem.at[1, i], back)

    def relay_two(i):
        return remote(rq.at[i, 2], rq.at[i, 4], m_sent.at[2], m_sem.at[2, i], back)

    def halo(direction, h, device, src=None):
        return remote(
            kvo.at[h] if src is None else src,
            kvh.at[direction, h],
            halo_sent.at[0 if src is None else 1],
            halo_sem.at[direction, h],
            device,
        )

    down = {"tm": me, "tile": tile + 1}
    up = {"tm": me, "tile": tile - 1}

    def opposite(n):
        return {"tm": across, "tile": n}

    def halo_out(h):
        @pl.when(has_down & jnp.logical_not(detours & (tile == upper)))
        def _():
            halo(0, h, down).start()

        @pl.when(has_up & jnp.logical_not(detours & (tile == lower)))
        def _():
            halo(1, h, up).start()

        by_last = (at_end & (tile == upper)) | (jnp.logical_not(at_end) & (tile == lower))

        @pl.when(detours & by_last)
        def _():
            halo(1, h, opposite(last)).start()

        @pl.when(detours & jnp.logical_not(by_last))
        def _():
            halo(0, h, opposite(0)).start()

    def halo_relay(h):
        for held, edge in ((0, 0), (1, last)):

            @pl.when(relays & (tile == edge))
            def _():
                halo(held, h, partner).wait_recv()

            for end in (True, False):
                onto = held if end else 1 - held

                @pl.when(relays & (tile == edge) & (at_end if end else jnp.logical_not(at_end)))
                def _():
                    halo(onto, h, opposite(upper if onto else lower), kvh.at[held, h]).start()

    def halo_in(h):
        @pl.when(has_up)
        def _():
            halo(0, h, partner).wait_recv()

        @pl.when(has_down)
        def _():
            halo(1, h, partner).wait_recv()

    slots = ((3, 5), (1, 3), (0, 1))

    def out_send(which, i):
        lo, hi = slots[which]
        return (
            remote(so.at[i, lo:hi], ro.at[i, lo:hi], n_sent.at[which], n_sem.at[which, i], ahead),
            remote(sl.at[i, lo:hi], rl.at[i, lo:hi], l_sent.at[which], l_sem.at[which, i], ahead),
        )

    def join(which, i):
        @pl.when(has_back)
        def _():
            for copy in out_send(which, i):
                copy.wait_recv()

    def far(i, which):
        lo, hi = slots[which]
        h = i // 2
        width = (hi - lo) * HD
        queries = rq[i, lo:hi].reshape(width, HD)
        seen = []
        for side in (2, 1):
            flags = [rm[j, j + side : j + side + 1, :] > 0.5 for j in range(lo, hi)]
            seen.append(jnp.concatenate([jnp.where(f, 1.0, 0.0) for f in flags], axis=1) > 0.5)
        parts = []
        for x in range(2):
            scores = scores_of(kvo[h, 0, x], queries)
            parts.append((scores, vt[h, x], [(0, scores.shape[0], seen[x])]))
        out, total, top = attend(parts)
        lse, scale = settle(total, top)
        if which:
            join(which - 1, i)
        for n, j in enumerate(range(lo, hi)):
            lanes = slice(n * HD, (n + 1) * HD)
            part, own_lse, own_scale = out[:, lanes], lse[:, lanes], scale[:, lanes]
            if which:
                wa, wb, new_lse = merge(own_lse, rl[i, j + 2])
                part = part * (own_scale * wa) + ro[i, j + 2].astype(jnp.float32) * wb
                own_lse = new_lse
            else:
                part = part * own_scale
            so[i, j] = part.astype(jnp.bfloat16)
            sl[i, j] = own_lse
        @pl.when(has_ahead)
        def _():
            for copy in out_send(which, i):
                copy.start()

    def near(h, f, x):
        queries = qo[h, f, x]
        second = jnp.full((1, HD), f, jnp.int32) > 0
        first = jnp.full((1, HD), f, jnp.int32) >= 0
        half = kvo.shape[3] // 2
        parts = [
            (scores_of(kvo[h, 0, x], queries), vt[h, x], [(0, half, first), (half, half, second)])
        ]
        for direction, reach in ((0, om[x, 0:1, :]), (1, om[x, 7:8, :])):
            groups = []
            for frame in range(2):
                for row in range(2):
                    need = 2 - row if direction == 0 else 1 + row
                    seen = reach > need - 0.5
                    if frame:
                        seen = seen & second
                    groups.append((frame * half + row * half // 2, half // 2, seen))
            parts.append((scores_of(kvh[direction, h, 0, x], queries), vth[direction, x], groups))
        if x == 1:
            parts.append(
                (scores_of(kvo[h, 0, 0], queries), vt[h, 0], [(0, 2 * half, om[1, 1:2, :] > 0.5)])
            )
        return queries, parts

    def give_out(h, f):
        pltpu.make_async_copy(
            outs.at[h, f, core], out_ref.at[f, :, column(core, h)], out_sem.at[0]
        ).start()
        remote(
            outs.at[h, f, other],
            out_ref.at[f, :, column(core, h)],
            out_sem.at[1],
            out_sem.at[2],
            partner,
        ).start()

    def own(i):
        h, f = i // 2, i % 2
        for x in range(2):
            _, parts = near(h, f, x)
            out, total, top = attend(parts)
            lse, scale = settle(total, top)
            if x == 0:
                join(2, i)
            wa, wb, _ = merge(lse, rl[i, x])
            whole = out * (scale * wa) + ro[i, x].astype(jnp.float32) * wb
            outs[h, f, x] = whole.T.astype(jnp.bfloat16)
        give_out(h, f)

    def own_by_keys(f):
        for x in range(2):
            queries, parts = near(kv_head, f, x)
            for distance in range(1 + x, 6):
                n, side = divmod(distance - 1 - x, 2)
                seen = om[x, distance : distance + 1, :] > 0.5
                scores = scores_of(rk[n, 0, 1 - side], queries)
                parts.append((scores, rk[n, 1, 1 - side].T, [(0, scores.shape[0], seen)]))
            out, total, _ = attend(parts)
            outs[kv_head, f, x] = (out * (1.0 / total)).T.astype(jnp.bfloat16)
        give_out(kv_head, f)

    def turn_values(h):
        for x in range(2):
            vt[h, x] = kvo[h, 1, x].T

    def turn_halo(h):
        for direction in range(2):
            for x in range(2):
                vth[direction, x] = kvh[direction, h, 1, x].T

    def during(t, lag):
        i = t - lag
        return i, (i >= 0) & (i < chunks)

    def key_send(n, i):
        src, dst = (
            (kvo.at[kv_head, i], rk.at[0, i]),
            (rk.at[0, i], rk.at[1, i]),
            (rk.at[1, i, 1], rk.at[2, i, 1]),
        )[n]
        return remote(src, dst, k_sent.at[n], k_sem.at[n, i], ahead)

    def pass_ahead(n, i):
        if n:

            @pl.when(has_back)
            def _():
                key_send(n - 1, i).wait_recv()

        @pl.when(has_ahead)
        def _():
            key_send(n, i).start()

    sends = (own_send, relay_one, relay_two)

    def pass_back(t, n):
        i, live = during(t, LAGS[n - 1] if n else -AHEAD)

        if n:

            @pl.when(live & has_ahead)
            def _():
                sends[n - 1](i).wait_recv()

                @pl.when(i == 0)
                def _():
                    meta_send(n - 1).wait_recv()

        @pl.when(live & has_back)
        def _():
            if n:

                @pl.when(i == 0)
                def _():
                    meta_send(n).start()

            sends[n](i).start()

    def step(t, _):
        @pl.when((t + AHEAD < chunks) & (t % 2 == 0))
        def _():
            await_queries((t + AHEAD) // 2)

        for n in (2, 1, 0):
            pass_back(t, n)

        @pl.when(t == 0)
        def _():
            arrived(kvo.at[:, :, core], kv_sem.at[0])
            arrived(kvo.at[:, :, other], kv_sem.at[1])
            for i in range(2):
                pass_ahead(0, i)

        for n in range(2):
            for i in range(2):

                @pl.when(t == 2 * n + 2 + i)
                def _():
                    pass_ahead(n + 1, i)

        for lag, run in ((0, halo_out), (RELAY, halo_relay)):
            i = t - lag

            @pl.when((i >= 0) & (i < 2 * heads) & (i % 2 == 0))
            def _():
                run(lax.rem(i // 2 + kv_head, heads))

        i3, live3 = during(t, LAGS[2])

        @pl.when(live3)
        def _():
            @pl.when(i3 % 2 == 0)
            def _():
                turn_values(i3 // 2)

            @pl.when(has_ahead)
            def _():
                relay_two(i3).wait_recv()

                @pl.when(i3 == 0)
                def _():
                    meta_send(2).wait_recv()

            far(i3, 0)

        for which in (1, 2):
            i, live = during(t, LAGS[2 + which])

            @pl.when(live)
            def _():
                far(i, which)

        @pl.when(t == KV_STEP)
        def _():
            await_queries(kv_head)

            @pl.when(has_back)
            def _():
                for i in range(2):
                    key_send(2, i).wait_recv()

            halo_in(kv_head)
            turn_values(kv_head)
            turn_halo(kv_head)

        @pl.when((t >= KV_STEP) & (t < KV_STEP + 2))
        def _():
            own_by_keys(t - KV_STEP)

        i6, live6 = during(t, LAGS[5])

        @pl.when(live6)
        def _():
            h = i6 // 2

            @pl.when(i6 % 2 == 0)
            def _():
                halo_in(h)
                turn_halo(h)

            own(i6)

        return 0

    lax.fori_loop(0, chunks + LAGS[5], step, 0)

    arrived(om.at[core], x_sent.at[0])
    arrived(qo.at[:, :, core], x_sent.at[1])
    arrived(kvo.at[:, :, core], x_sent.at[2])

    @pl.when(has_back)
    def _():
        arrived(om, x_sent.at[3])
        arrived(rm.at[0:2], x_sent.at[4])
        arrived(rm.at[2], x_sent.at[5])
        arrived(qo.at[0:kv_head], m_sent.at[0])
        arrived(rq.at[:, 0:2], m_sent.at[1])
        arrived(rq.at[:, 2], m_sent.at[2])

    @pl.when(has_ahead)
    def _():
        arrived(rk.at[0], k_sent.at[0])
        arrived(rk.at[0], k_sent.at[1])
        arrived(rk.at[0, :, 1], k_sent.at[2])
        for which, (lo, hi) in enumerate(slots):
            arrived(so.at[:, lo:hi], n_sent.at[which])
            arrived(sl.at[:, lo:hi], l_sent.at[which])

    @pl.when(has_down & has_up)
    def _():
        arrived(kvh, halo_sent.at[0])

    @pl.when(jnp.logical_not(has_down & has_up))
    def _():
        arrived(kvo, halo_sent.at[0])

    @pl.when(relays)
    def _():
        arrived(kvo, halo_sent.at[1])

    for i in range(3):
        arrived(outs.at[:, :, 0], out_sem.at[i])


def local(blocks, tiles, queries, keys, values, neighbours, halo_rows):
    frames, rows, width, channels = queries.shape
    tokens = frames * rows * width
    heads = channels // HD // 2
    chunks = 2 * heads - 2
    half = tokens // 2
    bf16, f32 = jnp.bfloat16, jnp.float32
    dma = pltpu.SemaphoreType.DMA
    result = pl.pallas_call(
        functools.partial(kernel, blocks, tiles, heads),
        out_shape=jax.ShapeDtypeStruct((2, half, channels), bf16),
        in_specs=[pl.BlockSpec(memory_space=pl.ANY)] * 3
        + [pl.BlockSpec(memory_space=pltpu.SMEM)] * 2,
        out_specs=pl.BlockSpec(memory_space=pl.ANY),
        scratch_shapes=[
            pltpu.VMEM((heads, 2, 2, half, HD), bf16),
            pltpu.VMEM((heads, 2, 2, tokens, HD), bf16),
            pltpu.VMEM((2, heads, 2, 2, tokens, HD), bf16),
            pltpu.VMEM((heads, 2, HD, tokens), bf16),
            pltpu.VMEM((2, 2, HD, tokens), bf16),
            pltpu.VMEM((chunks, 5, half, HD), bf16),
            pltpu.VMEM((chunks, 5, HD, half), bf16),
            pltpu.VMEM((chunks, 5, 1, half), f32),
            pltpu.VMEM((chunks, 5, HD, half), bf16),
            pltpu.VMEM((chunks, 5, 1, half), f32),
            pltpu.VMEM((heads, 2, 2, half, HD), bf16),
            pltpu.VMEM((2, 8, HD), f32),
            pltpu.VMEM((5, 8, HD), f32),
            pltpu.VMEM((3, 2, 2, tokens, HD), bf16),
            dma((heads,)),
            dma((heads,)),
            dma((2,)),
            dma((4,)),
            dma((2, heads)),
            dma((3, chunks)),
            dma((3, chunks)),
            dma((3, chunks)),
            dma((3,)),
            dma((3,)),
            dma((3,)),
            dma((6,)),
            dma((2,)),
            dma((3, 2)),
            dma((3,)),
            dma((3,)),
        ],
        compiler_params=pltpu.CompilerParams(
            collective_id=0, has_side_effects=True, vmem_limit_bytes=62 * 1024 * 1024
        ),
    )(
        queries.reshape(2, half, channels),
        keys.reshape(tokens, channels),
        values.reshape(tokens, channels),
        neighbours.reshape(-1),
        halo_rows.reshape(-1),
    )
    return result.reshape(frames, rows, width, channels)


def solution(mesh):
    body = functools.partial(local, mesh.shape["tm"], mesh.shape["tile"])
    return jax.shard_map(
        body,
        mesh=mesh,
        in_specs=(
            P("tm", "tile", None, None),
            P("tm", "tile", None, None),
            P("tm", "tile", None, None),
            P("tm", "tile", None),
            P("tm", "tile"),
        ),
        out_specs=P("tm", "tile", None, None),
        check_vma=False,
    )
```

```python
import functools
import math

import jax
import jax.numpy as jnp
from jax import lax
from jax.experimental import pallas as pl
from jax.experimental.pallas import tpu as pltpu
from jax.sharding import PartitionSpec as P

HD = 128
BIG = 1e30
SCALE = math.log2(math.e) / math.sqrt(HD)
AHEAD = 2
KV_STEP = 6
LAGS = (0,2,3,5,7,9)
RELAY = 3
OWN = 8
MESH = pl.DeviceIdType.MESH


def attend(parts):
    top = None
    for scores, _, groups in parts:
        for start, size, seen in groups:
            peak = jnp.max(scores[start : start + size], axis=0, keepdims=True)
            peak = jnp.where(seen, peak, -BIG)
            top = peak if top is None else jnp.maximum(top, peak)
    total, out = None, None
    for scores, value_t, groups in parts:
        pieces = []
        for start, size, seen in groups:
            shift = jnp.where(seen, top, BIG)
            weights = jnp.exp2((scores[start : start + size] - shift) * SCALE)
            added = jnp.sum(weights, axis=0, keepdims=True)
            total = added if total is None else total + added
            pieces.append(weights.astype(jnp.bfloat16))
        weights = pieces[0] if len(pieces) == 1 else jnp.concatenate(pieces, axis=0)
        product = jnp.dot(value_t, weights, preferred_element_type=jnp.float32)
        out = product if out is None else out + product
    return out, total, top


def scores_of(keys, queries):
    return lax.dot_general(
        keys, queries, (((1,), (1,)), ((), ())), preferred_element_type=jnp.float32
    )


def settle(total, top):
    empty = total == 0.0
    lse = jnp.where(empty, -BIG, top * SCALE + jnp.log2(jnp.where(empty, 1.0, total)))
    return lse, 1.0 / jnp.where(empty, 1.0, total)


def merge(lse_a, lse_b):
    top = jnp.maximum(lse_a, lse_b)
    wa, wb = jnp.exp2(lse_a - top), jnp.exp2(lse_b - top)
    both = wa + wb
    return wa / both, wb / both, top + jnp.log2(both)


def kernel(
    blocks,
    tiles,
    heads,
    q_ref,
    k_ref,
    v_ref,
    list_ref,
    reach_ref,
    out_ref,
    qo,
    kvo,
    kvh,
    vt,
    vth,
    rq,
    ro,
    rl,
    so,
    sl,
    outs,
    fp,
    fl,
    op,
    ol,
    om,
    rm,
    rk,
    q_local,
    q_remote,
    kv_sem,
    meta_sem,
    halo_sem,
    m_sem,
    n_sem,
    l_sem,
    m_sent,
    n_sent,
    l_sent,
    x_sent,
    halo_sent,
    k_sem,
    k_sent,
    out_sem,
):
    kv_head = heads - 1
    chunks = 2 * kv_head
    me = lax.axis_index("tm")
    tile = lax.axis_index("tile")
    core = lax.rem(me, 2)
    other = 1 - core
    partner = {"tm": me + 1 - 2 * core}
    back = {"tm": lax.rem(me + blocks - 2, blocks)}
    ahead = {"tm": lax.rem(me + 2, blocks)}
    across = lax.rem(me + blocks // 2, blocks)
    has_up = tile > 0
    has_down = tile < tiles - 1
    has_ahead = me < blocks - 2
    has_back = me >= 2
    upper, lower, last = tiles // 2 - 1, tiles // 2, tiles - 1
    chip = me // 2
    chips = blocks // 2
    at_end = (chip == 0) | (chip == chips - 1)
    at_edge = at_end | (chip == chips // 2 - 1) | (chip == chips // 2)
    detours = at_edge & ((tile == upper) | (tile == lower))
    relays = at_edge & ((tile == 0) | (tile == last))
    takes_up = has_up | (relays & (tile == 0))
    takes_down = has_down | (relays & (tile == last))

    def remote(src, dst, sent, received, device):
        return pltpu.make_async_remote_copy(
            src_ref=src,
            dst_ref=dst,
            send_sem=sent,
            recv_sem=received,
            device_id=device,
            device_id_type=MESH,
        )

    def arrived(ref, sem):
        pltpu.make_async_copy(ref, ref, sem).wait()

    def column(half, h):
        return pl.ds(pl.multiple_of((half * heads + h) * HD, HD), HD)

    barrier = pltpu.get_barrier_semaphore()
    pl.semaphore_signal(barrier, inc=1, device_id=partner, device_id_type=MESH)
    beside = (
        (has_back, back),
        (has_ahead, ahead),
        (has_up, {"tile": lax.max(tile - 1, 0)}),
        (has_down, {"tile": lax.min(tile + 1, tiles - 1)}),
    )
    peers = 1
    for there, device in beside:
        peers = peers + jnp.where(there, 1, 0)

        @pl.when(there)
        def _():
            pl.semaphore_signal(barrier, inc=1, device_id=device, device_id_type=MESH)

    peers = peers + jnp.where(detours | relays, 2, 0)

    @pl.when(detours)
    def _():
        for n in (0, tiles - 1):
            pl.semaphore_signal(
                barrier, inc=1, device_id={"tm": across, "tile": n}, device_id_type=MESH
            )

    @pl.when(relays)
    def _():
        for n in (upper, lower):
            pl.semaphore_signal(
                barrier, inc=1, device_id={"tm": across, "tile": n}, device_id_type=MESH
            )

    def fetch_q(h, _):
        pltpu.make_async_copy(
            q_ref.at[:, :, column(core, h)], qo.at[h, :, core], q_local.at[h]
        ).start()
        return 0

    def fetch_kv(h, _):
        for i, ref in enumerate((k_ref, v_ref)):
            pltpu.make_async_copy(
                ref.at[:, column(core, h)], kvo.at[h, i, core], kv_sem.at[0]
            ).start()
        return 0

    lax.fori_loop(0, heads, fetch_q, 0)
    lax.fori_loop(0, heads, fetch_kv, 0)

    distance = lax.broadcasted_iota(jnp.int32, (8, HD), 0)
    meta = jnp.zeros((8, HD), jnp.float32)
    for n in range(list_ref.shape[0]):
        block = list_ref[n]
        meta = jnp.where(distance == jnp.where(block >= 0, me - block, 0), 1.0, meta)
    reach = reach_ref[0].astype(jnp.float32)
    meta = jnp.where(distance == 0, jnp.where(has_up, reach, 0.0), meta)
    meta = jnp.where(distance == 7, jnp.where(has_down, reach, 0.0), meta)
    om[core] = meta

    @pl.when(jnp.logical_not(has_ahead))
    def _():
        rm[...] = jnp.zeros(rm.shape, rm.dtype)

        def clear(i, _):
            rq[i] = jnp.zeros(rq.shape[1:], rq.dtype)
            return 0

        lax.fori_loop(0, chunks, clear, 0)

    @pl.when(jnp.logical_not(has_back))
    def _():
        def clear(i, _):
            ro[i] = jnp.zeros(ro.shape[1:], ro.dtype)
            rl[i] = jnp.full(rl.shape[1:], -BIG, rl.dtype)
            return 0

        lax.fori_loop(0, chunks, clear, 0)
        for n in range(rk.shape[0]):
            for i in range(2):
                rk[n, i] = jnp.zeros(rk.shape[2:], rk.dtype)

    pl.semaphore_wait(barrier, peers)

    remote(om.at[core], om.at[core], x_sent.at[0], meta_sem.at[0], partner).start()

    def give_q(h, _):
        remote(
            q_ref.at[:, :, column(other, h)], qo.at[h, :, core], x_sent.at[1], q_remote.at[h], partner
        ).start()
        return 0

    def give_kv(h, _):
        for i, ref in enumerate((k_ref, v_ref)):
            remote(
                ref.at[:, column(other, h)], kvo.at[h, i, core], x_sent.at[2], kv_sem.at[1], partner
            ).start()
        return 0

    lax.fori_loop(0, heads, give_q, 0)

    def own_send(i):
        return remote(qo.at[i // 2, i % 2], rq.at[i, 0:2], m_sent.at[0], m_sem.at[0, i], back)

    def meta_send(n):
        src, dst = ((om, rm.at[0:2]), (rm.at[0:2], rm.at[2:4]), (rm.at[2], rm.at[4]))[n]
        return remote(src, dst, x_sent.at[3 + n], meta_sem.at[1 + n], back)

    def await_queries(h):
        arrived(qo.at[h, :, core], q_local.at[h])
        arrived(qo.at[h, :, other], q_remote.at[h])

    for i in range(AHEAD):
        if i % 2 == 0:
            await_queries(i // 2)

        @pl.when(has_back)
        def _():
            own_send(i).start()

    lax.fori_loop(0, heads, give_kv, 0)
    arrived(om.at[other], meta_sem.at[0])

    @pl.when(has_back)
    def _():
        meta_send(0).start()

    @pl.when(jnp.logical_not(takes_up))
    def _():
        def clear(h, _):
            kvh[0, h] = jnp.zeros(kvh.shape[2:], kvh.dtype)
            return 0

        lax.fori_loop(0, heads, clear, 0)

    @pl.when(jnp.logical_not(takes_down))
    def _():
        def clear(h, _):
            kvh[1, h] = jnp.zeros(kvh.shape[2:], kvh.dtype)
            return 0

        lax.fori_loop(0, heads, clear, 0)

    def relay_one(i):
        return remote(rq.at[i, 0:2], rq.at[i, 2:4], m_sent.at[1], m_sem.at[1, i], back)

    def relay_two(i):
        return remote(rq.at[i, 2], rq.at[i, 4], m_sent.at[2], m_sem.at[2, i], back)

    def halo(direction, h, device, src=None):
        return remote(
            kvo.at[h] if src is None else src,
            kvh.at[direction, h],
            halo_sent.at[0 if src is None else 1],
            halo_sem.at[direction, h],
            device,
        )

    down = {"tm": me, "tile": tile + 1}
    up = {"tm": me, "tile": tile - 1}

    def opposite(n):
        return {"tm": across, "tile": n}

    def halo_out(h):
        @pl.when(has_down & jnp.logical_not(detours & (tile == upper)))
        def _():
            halo(0, h, down).start()

        @pl.when(has_up & jnp.logical_not(detours & (tile == lower)))
        def _():
            halo(1, h, up).start()

        by_last = (at_end & (tile == upper)) | (jnp.logical_not(at_end) & (tile == lower))

        @pl.when(detours & by_last)
        def _():
            halo(1, h, opposite(last)).start()

        @pl.when(detours & jnp.logical_not(by_last))
        def _():
            halo(0, h, opposite(0)).start()

    def halo_relay(h):
        for held, edge in ((0, 0), (1, last)):

            @pl.when(relays & (tile == edge))
            def _():
                halo(held, h, partner).wait_recv()

            for end in (True, False):
                onto = held if end else 1 - held

                @pl.when(relays & (tile == edge) & (at_end if end else jnp.logical_not(at_end)))
                def _():
                    halo(onto, h, opposite(upper if onto else lower), kvh.at[held, h]).start()

    def halo_in(h):
        @pl.when(has_up)
        def _():
            halo(0, h, partner).wait_recv()

        @pl.when(has_down)
        def _():
            halo(1, h, partner).wait_recv()

    slots = ((3, 5), (1, 3), (0, 1))

    def out_send(which, i):
        lo, hi = slots[which]
        return (
            remote(so.at[i, lo:hi], ro.at[i, lo:hi], n_sent.at[which], n_sem.at[which, i], ahead),
            remote(sl.at[i, lo:hi], rl.at[i, lo:hi], l_sent.at[which], l_sem.at[which, i], ahead),
        )

    def join(which, i):
        @pl.when(has_back)
        def _():
            for copy in out_send(which, i):
                copy.wait_recv()

    def far(i, lo, hi):
        h = i // 2
        queries = rq[i, lo:hi].reshape((hi - lo) * HD, HD)
        parts = []
        for x in range(2):
            side = 2 - x
            flags = [jnp.where(rm[j, j + side : j + side + 1, :] > 0.5, 1.0, 0.0) for j in range(lo, hi)]
            seen = (flags[0] if len(flags) == 1 else jnp.concatenate(flags, axis=1)) > 0.5
            scores = scores_of(kvo[h, 0, x], queries)
            parts.append((scores, vt[h, x], [(0, scores.shape[0], seen)]))
        out, total, top = attend(parts)
        lse, scale = settle(total, top)
        out = out * scale
        for n, j in enumerate(range(lo, hi)):
            lanes = slice(n * HD, (n + 1) * HD)
            yield j, out[:, lanes], lse[:, lanes]

    def send_ahead(i, which):
        @pl.when(has_ahead)
        def _():
            for copy in out_send(which, i):
                copy.start()

    def far_first(i):
        for j, part, lse in far(i, *slots[0]):
            so[i, j] = part.astype(jnp.bfloat16)
            sl[i, j] = lse
        send_ahead(i, 0)
        for which in (1, 2):
            for j, part, lse in far(i, *slots[which]):
                fp[i, j] = part
                fl[i, j] = lse

    def far_join(i, which):
        join(which - 1, i)
        for j in range(*slots[which]):
            wa, wb, lse = merge(fl[i, j], rl[i, j + 2])
            part = fp[i, j] * wa + ro[i, j + 2].astype(jnp.float32) * wb
            so[i, j] = part.astype(jnp.bfloat16)
            sl[i, j] = lse
        send_ahead(i, which)

    def near(h, f, x):
        queries = qo[h, f, x]
        second = jnp.full((1, HD), f, jnp.int32) > 0
        first = jnp.full((1, HD), f, jnp.int32) >= 0
        half = kvo.shape[3] // 2
        parts = [
            (scores_of(kvo[h, 0, x], queries), vt[h, x], [(0, half, first), (half, half, second)])
        ]
        for direction, reach in ((0, om[x, 0:1, :]), (1, om[x, 7:8, :])):
            groups = []
            for frame in range(2):
                for row in range(2):
                    need = 2 - row if direction == 0 else 1 + row
                    seen = reach > need - 0.5
                    if frame:
                        seen = seen & second
                    groups.append((frame * half + row * half // 2, half // 2, seen))
            parts.append((scores_of(kvh[direction, h, 0, x], queries), vth[direction, x], groups))
        if x == 1:
            parts.append(
                (scores_of(kvo[h, 0, 0], queries), vt[h, 0], [(0, 2 * half, om[1, 1:2, :] > 0.5)])
            )
        return queries, parts

    def give_out(h, f):
        pltpu.make_async_copy(
            outs.at[h, f, core], out_ref.at[f, :, column(core, h)], out_sem.at[0]
        ).start()
        remote(
            outs.at[h, f, other],
            out_ref.at[f, :, column(core, h)],
            out_sem.at[1],
            out_sem.at[2],
            partner,
        ).start()

    def own_first(i):
        h, f = i // 2, i % 2
        for x in range(2):
            _, parts = near(h, f, x)
            out, total, top = attend(parts)
            lse, scale = settle(total, top)
            op[i, x] = out * scale
            ol[i, x] = lse

    def own_join(i):
        h, f = i // 2, i % 2
        join(2, i)
        for x in range(2):
            wa, wb, _ = merge(ol[i, x], rl[i, x])
            whole = op[i, x] * wa + ro[i, x].astype(jnp.float32) * wb
            outs[h, f, x] = whole.T.astype(jnp.bfloat16)
        give_out(h, f)

    def own_by_keys(f):
        for x in range(2):
            queries, parts = near(kv_head, f, x)
            for distance in range(1 + x, 6):
                n, side = divmod(distance - 1 - x, 2)
                seen = om[x, distance : distance + 1, :] > 0.5
                scores = scores_of(rk[n, 0, 1 - side], queries)
                parts.append((scores, rk[n, 1, 1 - side].T, [(0, scores.shape[0], seen)]))
            out, total, _ = attend(parts)
            outs[kv_head, f, x] = (out * (1.0 / total)).T.astype(jnp.bfloat16)
        give_out(kv_head, f)

    def turn_values(h):
        for x in range(2):
            vt[h, x] = kvo[h, 1, x].T

    def turn_halo(h):
        for direction in range(2):
            for x in range(2):
                vth[direction, x] = kvh[direction, h, 1, x].T

    def during(t, lag):
        i = t - lag
        return i, (i >= 0) & (i < chunks)

    def key_send(n, i):
        src, dst = (
            (kvo.at[kv_head, i], rk.at[0, i]),
            (rk.at[0, i], rk.at[1, i]),
            (rk.at[1, i, 1], rk.at[2, i, 1]),
        )[n]
        return remote(src, dst, k_sent.at[n], k_sem.at[n, i], ahead)

    def pass_ahead(n, i):
        if n:

            @pl.when(has_back)
            def _():
                key_send(n - 1, i).wait_recv()

        @pl.when(has_ahead)
        def _():
            key_send(n, i).start()

    sends = (own_send, relay_one, relay_two)

    def pass_back(t, n):
        i, live = during(t, LAGS[n - 1] if n else -AHEAD)

        if n:

            @pl.when(live & has_ahead)
            def _():
                sends[n - 1](i).wait_recv()

                @pl.when(i == 0)
                def _():
                    meta_send(n - 1).wait_recv()

        @pl.when(live & has_back)
        def _():
            if n:

                @pl.when(i == 0)
                def _():
                    meta_send(n).start()

            sends[n](i).start()

    def step(t, _):
        @pl.when((t + AHEAD < chunks) & (t % 2 == 0))
        def _():
            await_queries((t + AHEAD) // 2)

        for n in (2, 1, 0):
            pass_back(t, n)

        @pl.when(t == 0)
        def _():
            arrived(kvo.at[:, :, core], kv_sem.at[0])
            arrived(kvo.at[:, :, other], kv_sem.at[1])
            for i in range(2):
                pass_ahead(0, i)

        for n in range(2):
            for i in range(2):

                @pl.when(t == 2 * n + 2 + i)
                def _():
                    pass_ahead(n + 1, i)

        @pl.when(t < heads)
        def _():
            halo_out(lax.rem(t + kv_head, heads))

        i = t - RELAY

        @pl.when((i >= 0) & (i < 2 * heads) & (i % 2 == 0))
        def _():
            halo_relay(lax.rem(i // 2 + kv_head, heads))

        i3, live3 = during(t, LAGS[2])

        @pl.when(live3)
        def _():
            @pl.when(i3 % 2 == 0)
            def _():
                turn_values(i3 // 2)

            @pl.when(has_ahead)
            def _():
                relay_two(i3).wait_recv()

                @pl.when(i3 == 0)
                def _():
                    meta_send(2).wait_recv()

            far_first(i3)

        @pl.when(t == KV_STEP)
        def _():
            await_queries(kv_head)

            @pl.when(has_back)
            def _():
                for i in range(2):
                    key_send(2, i).wait_recv()

            halo_in(kv_head)
            turn_values(kv_head)
            turn_halo(kv_head)

        @pl.when((t >= KV_STEP) & (t < KV_STEP + 2))
        def _():
            own_by_keys(t - KV_STEP)

        i, live = during(t, OWN)

        @pl.when(live)
        def _():
            @pl.when(i % 2 == 0)
            def _():
                halo_in(i // 2)
                turn_halo(i // 2)

            own_first(i)

        for which in (1, 2):
            i, live = during(t, LAGS[2 + which])

            @pl.when(live)
            def _():
                far_join(i, which)

        i6, live6 = during(t, LAGS[5])

        @pl.when(live6)
        def _():
            own_join(i6)

        return 0

    lax.fori_loop(0, chunks + LAGS[5], step, 0)

    arrived(om.at[core], x_sent.at[0])
    arrived(qo.at[:, :, core], x_sent.at[1])
    arrived(kvo.at[:, :, core], x_sent.at[2])

    @pl.when(has_back)
    def _():
        arrived(om, x_sent.at[3])
        arrived(rm.at[0:2], x_sent.at[4])
        arrived(rm.at[2], x_sent.at[5])
        arrived(qo.at[0:kv_head], m_sent.at[0])
        arrived(rq.at[:, 0:2], m_sent.at[1])
        arrived(rq.at[:, 2], m_sent.at[2])

    @pl.when(has_ahead)
    def _():
        arrived(rk.at[0], k_sent.at[0])
        arrived(rk.at[0], k_sent.at[1])
        arrived(rk.at[0, :, 1], k_sent.at[2])
        for which, (lo, hi) in enumerate(slots):
            arrived(so.at[:, lo:hi], n_sent.at[which])
            arrived(sl.at[:, lo:hi], l_sent.at[which])

    @pl.when(has_down & has_up)
    def _():
        arrived(kvh, halo_sent.at[0])

    @pl.when(jnp.logical_not(has_down & has_up))
    def _():
        arrived(kvo, halo_sent.at[0])

    @pl.when(relays)
    def _():
        arrived(kvo, halo_sent.at[1])

    for i in range(3):
        arrived(outs.at[:, :, 0], out_sem.at[i])


def local(blocks, tiles, queries, keys, values, neighbours, halo_rows):
    frames, rows, width, channels = queries.shape
    tokens = frames * rows * width
    heads = channels // HD // 2
    chunks = 2 * heads - 2
    half = tokens // 2
    bf16, f32 = jnp.bfloat16, jnp.float32
    dma = pltpu.SemaphoreType.DMA
    result = pl.pallas_call(
        functools.partial(kernel, blocks, tiles, heads),
        out_shape=jax.ShapeDtypeStruct((2, half, channels), bf16),
        in_specs=[pl.BlockSpec(memory_space=pl.ANY)] * 3
        + [pl.BlockSpec(memory_space=pltpu.SMEM)] * 2,
        out_specs=pl.BlockSpec(memory_space=pl.ANY),
        scratch_shapes=[
            pltpu.VMEM((heads, 2, 2, half, HD), bf16),
            pltpu.VMEM((heads, 2, 2, tokens, HD), bf16),
            pltpu.VMEM((2, heads, 2, 2, tokens, HD), bf16),
            pltpu.VMEM((heads, 2, HD, tokens), bf16),
            pltpu.VMEM((2, 2, HD, tokens), bf16),
            pltpu.VMEM((chunks, 5, half, HD), bf16),
            pltpu.VMEM((chunks, 5, HD, half), bf16),
            pltpu.VMEM((chunks, 5, 1, half), f32),
            pltpu.VMEM((chunks, 5, HD, half), bf16),
            pltpu.VMEM((chunks, 5, 1, half), f32),
            pltpu.VMEM((heads, 2, 2, half, HD), bf16),
            pltpu.VMEM((chunks, 3, HD, half), f32),
            pltpu.VMEM((chunks, 3, 1, half), f32),
            pltpu.VMEM((chunks, 2, HD, half), f32),
            pltpu.VMEM((chunks, 2, 1, half), f32),
            pltpu.VMEM((2, 8, HD), f32),
            pltpu.VMEM((5, 8, HD), f32),
            pltpu.VMEM((3, 2, 2, tokens, HD), bf16),
            dma((heads,)),
            dma((heads,)),
            dma((2,)),
            dma((4,)),
            dma((2, heads)),
            dma((3, chunks)),
            dma((3, chunks)),
            dma((3, chunks)),
            dma((3,)),
            dma((3,)),
            dma((3,)),
            dma((6,)),
            dma((2,)),
            dma((3, 2)),
            dma((3,)),
            dma((3,)),
        ],
        compiler_params=pltpu.CompilerParams(
            collective_id=0, has_side_effects=True, vmem_limit_bytes=52 * 1024 * 1024
        ),
    )(
        queries.reshape(2, half, channels),
        keys.reshape(tokens, channels),
        values.reshape(tokens, channels),
        neighbours.reshape(-1),
        halo_rows.reshape(-1),
    )
    return result.reshape(frames, rows, width, channels)


def solution(mesh):
    body = functools.partial(local, mesh.shape["tm"], mesh.shape["tile"])
    return jax.shard_map(
        body,
        mesh=mesh,
        in_specs=(
            P("tm", "tile", None, None),
            P("tm", "tile", None, None),
            P("tm", "tile", None, None),
            P("tm", "tile", None),
            P("tm", "tile"),
        ),
        out_specs=P("tm", "tile", None, None),
        check_vma=False,
    )
```
